256 devices in a mesh: blk: 8 (over y, core), rep: 8 (over z), sub: 4 (over x).
Axes of the slice: x: 4, y: 4, z: 8, core: 2. Of those that a mesh axis runs over, the one named last changes fastest.
Arguments:
- image_embed: bfloat16 [16384, 1152], P(('blk', 'rep', 'sub')), may hold values from -60 to 60
- text_embed: bfloat16 [16384, 1152], P(('blk', 'rep', 'sub')), may hold values from -60 to 60
- image_ids: int32 [16384], P(('blk', 'rep', 'sub')), may hold values from 0 to 8191
- text_ids: int32 [16384], P(('blk', 'rep', 'sub')), may hold values from 0 to 8191
Outputs:
- image_grad: float32 [16384, 1152], P(('blk', 'rep', 'sub'))
- text_grad: float32 [16384, 1152], P(('blk', 'rep', 'sub'))
The draws below stay inside these ranges and needn't reach their ends.
All inputs are finite; a program needn't handle non-finite values.
Results may differ from the reference program's by a relative error of at most 0.008.
Values may be sent and summed in bfloat16 or wider, within the bound.
A program may use at most 64 MiB of HBM per device.

```python
import math
import jax
import jax.numpy as jnp
from jax import lax

D = 1152
TOKENS = 16384


def rough_rows(key, salt):
    key = jax.random.fold_in(key, salt)
    first, second = jax.random.split(key, 2)
    base = jnp.clip(jax.random.normal(first, (TOKENS, D), jnp.float32), -6.0, 6.0)
    scale = jnp.exp(jax.random.uniform(second, (TOKENS, 1), jnp.float32) * math.log(10.0))
    return (base * scale).astype(jnp.bfloat16)


def draw_image_embed(key, part):
    return rough_rows(key, 11)


def draw_text_embed(key, part):
    return rough_rows(key, 23)


def set_ends(array, key, smallest, top_value):
    spot = [jax.random.randint(jax.random.fold_in(key, axis), (), 0, length) for axis, length in enumerate(array.shape)]
    widest = array.shape.index(max(array.shape))
    next_to = spot[:widest] + [(spot[widest] + 1) % array.shape[widest]] + spot[widest + 1:]
    return array.at[tuple(spot)].set(smallest).at[tuple(next_to)].set(top_value)


def setup_inputs(seed: int = 0) -> dict:
    seeds = jax.random.split(jax.random.key(seed), 5)
    return {
        "image_embed": draw_image_embed(jax.random.fold_in(seeds[4], 71), 0),
        "text_embed": draw_text_embed(jax.random.fold_in(seeds[4], 71), 0),
        "image_ids": set_ends(jax.random.randint(seeds[2], (TOKENS,), 0, TOKENS // 2), jax.random.fold_in(seeds[2], 1), 0, (TOKENS // 2) - 1).astype(jnp.int32),
        "text_ids": set_ends(jax.random.randint(seeds[3], (TOKENS,), 0, TOKENS // 2), jax.random.fold_in(seeds[3], 1), 0, (TOKENS // 2) - 1).astype(jnp.int32),
    }


logit_scale = 30.0
logit_bias = -3.0

def unit_rows(embed):
    values = embed.astype(jnp.float32)
    inverse = lax.rsqrt(lax.optimization_barrier(jnp.sum(values * values, axis=1, keepdims=True)) + 1e-06)
    return (values * inverse, inverse)

def project(unit, inverse, grad):
    along = lax.optimization_barrier(jnp.sum(unit * grad, axis=1, keepdims=True))
    return (grad - unit * along) * inverse

def reference(image_embed, text_embed, image_ids, text_ids):
    img_unit, img_inv = unit_rows(image_embed)
    txt_unit, txt_inv = unit_rows(text_embed)
    img_half = img_unit.astype(jnp.bfloat16)
    text_subset = txt_unit.astype(jnp.bfloat16)
    block = math.gcd(TOKENS, 1024)
    img_blocks = img_half.reshape(TOKENS // block, block, D)
    id_blocks = image_ids.reshape(TOKENS // block, block)

    def step(carry, item):
        batch_rows, keys = item
        pair_logits = logit_scale * jnp.dot(batch_rows, text_subset.T, preferred_element_type=jnp.float32) + logit_bias
        label_sign = (keys[:, None] == text_ids[None, :]).astype(jnp.float32)
        gradient_factor = (logit_scale * (jax.nn.sigmoid(pair_logits) - label_sign)).astype(jnp.bfloat16)
        grad_rows = jnp.dot(gradient_factor, text_subset, preferred_element_type=jnp.float32)
        carry = carry + lax.dot_general(gradient_factor, batch_rows, (((0,), (0,)), ((), ())), preferred_element_type=jnp.float32)
        return (carry, grad_rows)
    start = jnp.zeros((TOKENS, D), jnp.float32)
    g_txt, g_img = lax.scan(step, start, (img_blocks, id_blocks))
    g_img = g_img.reshape(TOKENS, D)
    return (project(img_unit, img_inv, g_img), project(txt_unit, txt_inv, g_txt))
```

```python
import jax
import jax.numpy as jnp
from jax import lax
from jax.experimental import pallas as pl
from jax.experimental.pallas import tpu as pltpu
from jax.sharding import PartitionSpec as P

SCALE = 30.0
BIAS = -3.0
ROWS = 64
D = 1152
MESH = pl.DeviceIdType.MESH
F32 = jnp.float32
BF16 = jnp.bfloat16

Z_ORDER = (4, 3, -3, 2, -2, 1, -1, 0)
T_ORDER = (
    (2, 2), (1, 2), (2, 1), (-1, 2), (2, -1), (0, 2), (2, 0), (1, 1),
    (-1, 1), (1, -1), (-1, -1), (0, 1), (1, 0), (0, -1), (-1, 0), (0, 0),
)
RING4 = (0, 1, -1, 2)


def near4(d):
    return (d + 1) % 4 - 1


def near8(d):
    return (d + 3) % 8 - 3


def img_row(lane, dz):
    return Z_ORDER.index(near8(dz)) * 128 + lane * 64


def txt_row(dx, dy):
    return T_ORDER.index((near4(dx), near4(dy))) * 64


def tid_row(dx, dy):
    return RING4.index(near4(dy)) * 4 + RING4.index(near4(dx))


def iid_row(dz):
    return Z_ORDER.index(near8(dz)) * 2


class Plan:
    def __init__(self):
        self.msgs = {}
        self.origin = {}
        self.rows = {"sb": 0, "rb": 0}

    def add(self, name, way, src, dst, terms=None):
        self.msgs[name] = (len(self.msgs), way, src, dst, terms)
        buf, row, n = dst
        for r in range(row, row + n):
            assert (buf, r) not in self.origin
            self.origin[(buf, r)] = name

    def room(self, buf, n):
        row = self.rows[buf]
        self.rows[buf] += n
        return row

    def reduce(self, name, way, n, pieces):
        src, dst = self.room("sb", n), self.room("rb", n)
        self.add(name, way, ("sb", src, n), ("rb", dst, n), pieces)
        return dst


def make_plan():
    p = Plan()
    p.add("id", "c", ("iid", iid_row(0), 1), ("iid", iid_row(0) + 1, 1))
    for k in range(4):
        p.add(f"izp{k}", "z+", ("iid", iid_row(-k), 2), ("iid", iid_row(-k - 1), 2))
        if k < 3:
            p.add(f"izm{k}", "z-", ("iid", iid_row(k), 2), ("iid", iid_row(k + 1), 2))
    p.add("itxp0", "x+", ("tid", tid_row(0, 0), 1), ("tid", tid_row(-1, 0), 1))
    p.add("itxm0", "x-", ("tid", tid_row(0, 0), 1), ("tid", tid_row(1, 0), 1))
    p.add("itxp1", "x+", ("tid", tid_row(-1, 0), 1), ("tid", tid_row(2, 0), 1))
    p.add("ityp0", "y+", ("tid", tid_row(0, 0), 4), ("tid", tid_row(0, -1), 4))
    p.add("itym0", "y-", ("tid", tid_row(0, 0), 4), ("tid", tid_row(0, 1), 4))
    p.add("ityp1", "y+", ("tid", tid_row(0, -1), 4), ("tid", tid_row(0, 2), 4))
    for k in range(4):
        for h in (0, 1):
            if k < 3 or h == 0:
                p.add(f"zp{k}{h}", "z+", ("img", img_row(0, -k) + 32 * h, 32),
                      ("img", img_row(0, -k - 1) + 32 * h, 32))
            if k < 3 or h == 1:
                p.add(f"zm{k}{h}", "z-", ("img", img_row(0, k) + 32 * h, 32),
                      ("img", img_row(0, k + 1) + 32 * h, 32))
    for dz in Z_ORDER:
        p.add(f"d{dz}", "c", ("img", img_row(0, dz), 64), ("img", img_row(1, dz), 64))
    for half, one, two, at in (("a", "x", "y", lambda u, v: txt_row(u, v)), ("b", "y", "x", lambda u, v: txt_row(v, u))):
        o = 0 if half == "a" else 32
        p.add(f"{half}1p0", one + "+", ("txt", at(0, 0) + o, 32), ("txt", at(-1, 0) + o, 32))
        p.add(f"{half}1m0", one + "-", ("txt", at(0, 0) + o, 32), ("txt", at(1, 0) + o, 32))
        p.add(f"{half}1p1", one + "+", ("txt", at(-1, 0) + o, 16), ("txt", at(2, 0) + o, 16))
        p.add(f"{half}1m1", one + "-", ("txt", at(1, 0) + o + 16, 16), ("txt", at(2, 0) + o + 16, 16))
        for u in RING4:
            p.add(f"{half}2p0{u}", two + "+", ("txt", at(u, 0) + o, 32), ("txt", at(u, -1) + o, 32))
            p.add(f"{half}2m0{u}", two + "-", ("txt", at(u, 0) + o, 32), ("txt", at(u, 1) + o, 32))
            p.add(f"{half}2p1{u}", two + "+", ("txt", at(u, -1) + o, 16), ("txt", at(u, 2) + o, 16))
            p.add(f"{half}2m1{u}", two + "-", ("txt", at(u, 1) + o + 16, 16), ("txt", at(u, 2) + o + 16, 16))
    part = {}
    for dz in Z_ORDER:
        part[dz] = p.reduce(f"e{dz}", "c", 64, [(0, 64, [("gi", img_row(1, dz))])])
    got = {}
    for s, way in ((1, "z+"), (-1, "z-")):
        c = "p" if s == 1 else "m"
        for j in (4, 3, 2, 1):
            dz = near8(s * j)
            for h in ((0, 1) if s == 1 else (1, 0)):
                if j == 4 and h != (0 if s == 1 else 1):
                    continue
                terms = [("gi", img_row(0, dz) + 32 * h), ("rb", part[dz] + 32 * h)]
                if (s, j, h) in got:
                    terms.append(("rb", got[(s, j, h)]))
                got[(s, j - 1, h)] = p.reduce(f"rz{c}{j}{h}", way, 32, [(0, 32, terms)])
    p.final_img = [
        (32 * h, 32, [("gi", img_row(0, 0) + 32 * h), ("rb", part[0] + 32 * h),
                      ("rb", got[(1, 0, h)]), ("rb", got[(-1, 0, h)])])
        for h in (0, 1)
    ]
    p.final_txt = []
    for half, one, two, at in (("a", "x", "y", lambda u, v: txt_row(u, v)), ("b", "y", "x", lambda u, v: txt_row(v, u))):
        o = 0 if half == "a" else 32
        base = {}
        for u in RING4:
            far, last = {}, {}
            for s, c, q in ((1, "p", 0), (-1, "m", 16)):
                far[s] = p.reduce(f"r{half}2{c}2{u}", f"{two}{'+' if s == 1 else '-'}", 16,
                                  [(0, 16, [("gt", at(u, 2) + o + q)])])
            for s, c, q in ((1, "p", 0), (-1, "m", 16)):
                pieces = [(f, 16, [("gt", at(u, s) + o + f)] + ([("rb", far[s])] if f == q else [])) for f in (0, 16)]
                last[s] = p.reduce(f"r{half}2{c}1{u}", f"{two}{'+' if s == 1 else '-'}", 32, pieces)
            base[u] = [[("gt", at(u, 0) + o + f), ("rb", last[1] + f), ("rb", last[-1] + f)] for f in (0, 16)]
        far, last = {}, {}
        for s, c, q in ((1, "p", 0), (-1, "m", 16)):
            far[s] = p.reduce(f"r{half}1{c}2", f"{one}{'+' if s == 1 else '-'}", 16, [(0, 16, base[2][q // 16])])
        for s, c, q in ((1, "p", 0), (-1, "m", 16)):
            pieces = [(f, 16, base[s][f // 16] + ([("rb", far[s])] if f == q else [])) for f in (0, 16)]
            last[s] = p.reduce(f"r{half}1{c}1", f"{one}{'+' if s == 1 else '-'}", 32, pieces)
        p.final_txt += [(o + f, 16, base[0][f // 16] + [("rb", last[1] + f), ("rb", last[-1] + f)]) for f in (0, 16)]
    return p


PLAN = make_plan()


def both(stem, *tails):
    return [f"{stem}{c}{t}" for t in tails for c in "pm"]


def schedule():
    s = []
    send = lambda *names: s.append(("send", names))
    send("id", "itxp0", "itxm0")
    send("a1p0", "a1m0", "b1p0", "b1m0", "zp00", "zm01", "zp01", "zm00")
    send("a2p00", "a2m00", "b2p00", "b2m00", "d0")
    send("izp0", "izm0", "itxp1")
    send("zp10", "zm11")
    send("a1p1", "a1m1", "b1p1", "b1m1")
    for u in (-1, 1):
        send(*both("a2", f"0{u}"), *both("b2", f"0{u}"))
    send("ityp0", "itym0", "izp1", "izm1")
    send("zp11", "zm10", "d-1", "d1")
    send("ityp1", "izp2", "izm2", "izp3")
    send(*both("a2", "02"), *both("b2", "02"))
    send(*both("a2", "10"), *both("b2", "10"))
    send("zp20", "zm21")
    s.append(("tile", 3, 3))
    send(*both("a2", "1-1"), *both("b2", "1-1"))
    send("zp21", "zm20", "d-2", "d2")
    send(*both("a2", "11"), *both("b2", "11"))
    s.append(("tile", 3, 2))
    send("zp30", "zm31")
    s.append(("tile", 2, 3))
    send(*both("a2", "12"), *both("b2", "12"))
    s.append(("tile", 2, 2))
    send("d-3", "d3")
    s.append(("tile", 1, 3))
    s.append(("tile", 1, 2))
    s.append(("tile", 3, 1))
    s.append(("tile", 2, 1))
    send("d4")
    s.append(("tile", 1, 1))
    s.append(("tile", 3, 0))
    s.append(("tile", 2, 0))
    s.append(("tile", 1, 0))
    for t in (3, 2, 1, 0):
        s.append(("tile", 0, t))
    s.append(("gi", 0))
    send("e4", "e3")
    s.append(("gt", 0))
    for u in (2, 1):
        send(*both("ra2", f"2{u}"), *both("rb2", f"2{u}"))
    send(*both("ra2", "2-1"))
    send("rzp40", "rzm41", "rzp31")
    s.append(("gt", 1))
    send(*both("rb2", "2-1"), *both("ra2", "20"), *both("rb2", "20"))
    s.append(("gi", 1))
    send("e-3", "e2")
    send(*both("ra2", "12"), *both("rb2", "12"))
    send("rzm30", "rzp30", "rzm31")
    s.append(("gt", 2))
    send(*both("ra2", "11"), *both("rb2", "11"))
    s.append(("gi", 2))
    send("e-2", "e1")
    send("rzp21", "rzm20")
    s.append(("gt", 3))
    send(*both("ra2", "1-1"), *both("rb2", "1-1"))
    send("rzp20", "rzm21")
    s.append(("gi", 3))
    send("e-1", "e0")
    send("rzp11", "rzm10")
    send(*both("ra1", "2"), *both("rb1", "2"))
    send(*both("ra2", "10"), *both("rb2", "10"))
    send("rzp10", "rzm11")
    send(*both("ra1", "1"), *both("rb1", "1"))
    s.append(("out", "i"))
    s.append(("out", "t"))
    return s


def kernel(ie_ref, te_ref, ii_ref, ti_ref, oi_ref, ot_ref,
           img, txt, coef, gi, gt, sb, rb, iid, tid, icol, ssem, rsem):
    blk, rep, sub = lax.axis_index("blk"), lax.axis_index("rep"), lax.axis_index("sub")
    where = {
        "x+": {"sub": lax.rem(sub + 1, 4)}, "x-": {"sub": lax.rem(sub + 3, 4)},
        "y+": {"blk": lax.rem(blk + 2, 8)}, "y-": {"blk": lax.rem(blk + 6, 8)},
        "z+": {"rep": lax.rem(rep + 1, 8)}, "z-": {"rep": lax.rem(rep + 7, 8)},
        "c": {"blk": blk + 1 - 2 * lax.rem(blk, 2)},
    }
    barrier = pltpu.get_barrier_semaphore()
    for way in where.values():
        pl.semaphore_signal(barrier, inc=1, device_id=way, device_id_type=MESH)

    def unit(ref):
        v = ref[...].astype(F32)
        inv = lax.rsqrt(jnp.sum(v * v, axis=1, keepdims=True) + 1e-6)
        return v * inv, inv

    img[pl.ds(img_row(0, 0), ROWS), :] = unit(ie_ref)[0].astype(BF16)
    txt[pl.ds(txt_row(0, 0), ROWS), :] = unit(te_ref)[0].astype(BF16)
    for ids, ref, row in ((ii_ref, iid, iid_row(0)), (ti_ref, tid, tid_row(0, 0))):
        ref[row] = jnp.concatenate([ids[...], ids[...]], axis=1)
    pl.semaphore_wait(barrier, len(where))

    bufs = {"img": img, "txt": txt, "gi": gi, "gt": gt, "sb": sb, "rb": rb, "iid": iid, "tid": tid}

    def copy(name):
        index, way, src, dst, _ = PLAN.msgs[name]
        return pltpu.make_async_remote_copy(
            src_ref=bufs[src[0]].at[pl.ds(src[1], src[2])],
            dst_ref=bufs[dst[0]].at[pl.ds(dst[1], dst[2])],
            send_sem=ssem.at[index], recv_sem=rsem.at[index],
            device_id=where[way], device_id_type=MESH,
        )

    here, sent = set(), []

    def need(buf, row, n):
        for r in range(row, row + n):
            name = PLAN.origin.get((buf, r))
            if name is not None and name not in here:
                here.add(name)
                copy(name).wait_recv()

    def total(n, terms):
        acc = None
        for buf, row in terms:
            need(buf, row, n)
            v = bufs[buf][pl.ds(row, n), :].astype(F32)
            acc = v if acc is None else acc + v
        return acc

    def send(name):
        _, _, src, _, pieces = PLAN.msgs[name]
        if pieces is None:
            need(*src)
        else:
            for off, n, terms in pieces:
                sb[pl.ds(src[1] + off, n), :] = total(n, terms).astype(BF16)
        copy(name).start()
        sent.append(name)

    lane = lax.broadcasted_iota(jnp.int32, (1, 128), 1)
    ready = set()

    def columns(i):
        if i in ready:
            return
        ready.add(i)
        for p in (2 * i, 2 * i + 1):
            need("iid", 2 * p, 2)
            both_ids = jnp.where(lane < 64, iid[2 * p], iid[2 * p + 1])
            icol[pl.ds(128 * p, 128), :] = jnp.transpose(jnp.broadcast_to(both_ids, (128, 128)))

    def tile(i, t):
        need("img", 256 * i, 256)
        need("txt", 256 * t, 256)
        columns(i)
        keys = []
        for b in (4 * t, 4 * t + 2):
            r0, r1 = tid_row(*T_ORDER[b]), tid_row(*T_ORDER[b + 1])
            need("tid", r0, 1)
            need("tid", r1, 1)
            keys.append(jnp.where(lane < 64, tid[r0], tid[r1]))
        z = lax.dot_general(img[pl.ds(256 * i, 256), :], txt[pl.ds(256 * t, 256), :],
                            (((1,), (1,)), ((), ())), preferred_element_type=F32)
        sig = jax.nn.sigmoid(SCALE * z + BIAS)
        rows = icol[pl.ds(256 * i, 256), :]
        same = jnp.concatenate([(rows == k).astype(F32) for k in keys], axis=1)
        coef[pl.ds(256 * i, 256), pl.ds(256 * t, 256)] = (SCALE * (sig - same)).astype(BF16)

    def finish(pieces, ref, out):
        u, inv = unit(ref)
        for off, n, terms in pieces:
            g = total(n, terms)
            uu = u[off:off + n]
            along = jnp.sum(uu * g, axis=1, keepdims=True)
            out[pl.ds(off, n), :] = (g - uu * along) * inv[off:off + n]

    for step in schedule():
        if step[0] == "send":
            for name in step[1]:
                send(name)
        elif step[0] == "tile":
            tile(step[1], step[2])
        elif step[0] == "gi":
            rows = pl.ds(256 * step[1], 256)
            gi[rows, :] = jnp.dot(coef[rows, :], txt[...], preferred_element_type=F32)
        elif step[0] == "gt":
            rows = pl.ds(256 * step[1], 256)
            gt[rows, :] = lax.dot_general(coef[:, rows], img[...], (((0,), (0,)), ((), ())),
                                          preferred_element_type=F32)
        elif step[1] == "i":
            finish(PLAN.final_img, ie_ref, oi_ref)
        else:
            finish(PLAN.final_txt, te_ref, ot_ref)
    assert len(sent) == len(PLAN.msgs) and len(here) == len(PLAN.msgs)
    for name in sent:
        copy(name).wait_send()


def body(image_embed, text_embed, image_ids, text_ids):
    vmem = pl.BlockSpec(memory_space=pltpu.VMEM)
    n = len(PLAN.msgs)
    out = jax.ShapeDtypeStruct((ROWS, D), F32)
    return pl.pallas_call(
        kernel,
        name="pairs",
        out_shape=(out, out),
        in_specs=[vmem] * 4,
        out_specs=(vmem, vmem),
        scratch_shapes=[
            pltpu.VMEM((1024, D), BF16),
            pltpu.VMEM((1024, D), BF16),
            pltpu.VMEM((1024, 1024), BF16),
            pltpu.VMEM((1024, D), F32),
            pltpu.VMEM((1024, D), F32),
            pltpu.VMEM((PLAN.rows["sb"], D), BF16),
            pltpu.VMEM((PLAN.rows["rb"], D), BF16),
            pltpu.VMEM((16, 1, 128), jnp.int32),
            pltpu.VMEM((16, 1, 128), jnp.int32),
            pltpu.VMEM((1024, 128), jnp.int32),
            pltpu.SemaphoreType.DMA((n,)),
            pltpu.SemaphoreType.DMA((n,)),
        ],
        compiler_params=pltpu.CompilerParams(
            collective_id=0, has_side_effects=True, vmem_limit_bytes=60 * 1024 * 1024
        ),
    )(image_embed, text_embed, image_ids.reshape(1, ROWS), text_ids.reshape(1, ROWS))


def solution(mesh):
    rows = P(("blk", "rep", "sub"), None)
    flat = P(("blk", "rep", "sub"))
    return jax.shard_map(
        body, mesh=mesh, in_specs=(rows, rows, flat, flat), out_specs=(rows, rows), check_vma=False
    )
```

```python
import jax
import jax.numpy as jnp
from jax import lax
from jax.experimental import pallas as pl
from jax.experimental.pallas import tpu as pltpu
from jax.sharding import PartitionSpec as P

SCALE = 30.0
BIAS = -3.0
ROWS = 64
D = 1152
UNIT = 16
GATHER_XY, REDUCE_XY = 32, 32
PARTS_Z = {1: ((0, 16), (16, 16), (32, 16), (48, 16)), -1: ((48, 16), (32, 16), (16, 16), (0, 16))}
IMG_CHUNKS = ((0, 256), (256, 256), (512, 256), (768, 256))
TXT_CHUNKS = ((0, 256), (256, 256), (512, 256), (768, 256))
MESH = pl.DeviceIdType.MESH
F32 = jnp.float32
BF16 = jnp.bfloat16

Z_ORDER = (4, 3, -3, 2, -2, 1, -1, 0)
T_ORDER = (
    (2, 2), (1, 2), (2, 1), (-1, 2), (2, -1), (0, 2), (2, 0), (1, 1),
    (-1, 1), (1, -1), (-1, -1), (0, 1), (1, 0), (0, -1), (-1, 0), (0, 0),
)
RING4 = (0, 1, -1, 2)


def near4(d):
    return (d + 1) % 4 - 1


def near8(d):
    return (d + 3) % 8 - 3


def img_row(lane, dz):
    return Z_ORDER.index(near8(dz)) * 128 + lane * 64


def txt_row(dx, dy):
    return T_ORDER.index((near4(dx), near4(dy))) * 64


def tid_row(dx, dy):
    return RING4.index(near4(dy)) * 4 + RING4.index(near4(dx))


def iid_row(dz):
    return Z_ORDER.index(near8(dz)) * 2


class Plan:
    def __init__(self):
        self.msgs = []
        self.origin = {}
        self.rows = {"sb": 0, "rb": 0}

    def add(self, way, src, dst, pieces=None):
        buf, row, n = dst
        for r in range(row, row + n):
            assert (buf, r) not in self.origin
            self.origin[buf, r] = len(self.msgs)
        self.msgs.append((way, src, dst, pieces))

    def room(self, buf, n):
        row = self.rows[buf]
        self.rows[buf] += n
        return row

    def reduce(self, way, n, *pieces):
        src, dst = self.room("sb", n), self.room("rb", n)
        self.add(way, ("sb", src, n), ("rb", dst, n), pieces)
        return dst


SIDES = ((1, "+"), (-1, "-"))
HALVES = ((0, "x", "y", lambda u, v: txt_row(u, v)), (32, "y", "x", lambda u, v: txt_row(v, u)))


def make_plan():
    p = Plan()
    p.add("c", ("iid", iid_row(0), 1), ("iid", iid_row(0) + 1, 1))
    for k in range(4):
        p.add("z+", ("iid", iid_row(-k), 2), ("iid", iid_row(-k - 1), 2))
        if k < 3:
            p.add("z-", ("iid", iid_row(k), 2), ("iid", iid_row(k + 1), 2))
    p.add("x+", ("tid", tid_row(0, 0), 1), ("tid", tid_row(-1, 0), 1))
    p.add("x-", ("tid", tid_row(0, 0), 1), ("tid", tid_row(1, 0), 1))
    p.add("x+", ("tid", tid_row(-1, 0), 1), ("tid", tid_row(2, 0), 1))
    p.add("y+", ("tid", tid_row(0, 0), 4), ("tid", tid_row(0, -1), 4))
    p.add("y-", ("tid", tid_row(0, 0), 4), ("tid", tid_row(0, 1), 4))
    p.add("y+", ("tid", tid_row(0, -1), 4), ("tid", tid_row(0, 2), 4))
    for k in range(4):
        for s, w in SIDES:
            for q, n in PARTS_Z[s]:
                if k < 3 or (q < 32) == (s == 1):
                    p.add("z" + w, ("img", img_row(0, -s * k) + q, n), ("img", img_row(0, -s * (k + 1)) + q, n))
    for dz in Z_ORDER:
        for h in (0, 1):
            p.add("c", ("img", img_row(0, dz) + 32 * h, 32), ("img", img_row(1, dz) + 32 * h, 32))
    for o, one, two, at in HALVES:
        n = GATHER_XY
        for s, w in SIDES:
            for q in range(0, 32, n):
                p.add(one + w, ("txt", at(0, 0) + o + q, n), ("txt", at(-s, 0) + o + q, n))
                for u in RING4:
                    p.add(two + w, ("txt", at(u, 0) + o + q, n), ("txt", at(u, -s) + o + q, n))
            e = o if s == 1 else o + UNIT
            p.add(one + w, ("txt", at(-s, 0) + e, UNIT), ("txt", at(2, 0) + e, UNIT))
            for u in RING4:
                p.add(two + w, ("txt", at(u, -s) + e, UNIT), ("txt", at(u, 2) + e, UNIT))
    part = {}
    for dz in Z_ORDER:
        for h in (0, 1):
            row = p.reduce("c", 32, [("gi", img_row(1, dz) + 32 * h)])
            part[dz, 2 * h], part[dz, 2 * h + 1] = row, row + UNIT
    got = {}
    for j in (4, 3, 2, 1):
        for s, w in SIDES:
            for q, n in PARTS_Z[s]:
                if j == 4 and (q < 32) != (s == 1):
                    continue
                dz, pieces = near8(s * j), []
                for e in range(q // UNIT, (q + n) // UNIT):
                    terms = [("gi", img_row(0, dz) + UNIT * e), ("rb", part[dz, e])]
                    if (s, j, e) in got:
                        terms.append(("rb", got[s, j, e]))
                    pieces.append(terms)
                row = p.reduce("z" + w, n, *pieces)
                for k in range(n // UNIT):
                    got[s, j - 1, q // UNIT + k] = row + UNIT * k
    p.final_img = [
        (UNIT * q, [("gi", img_row(0, 0) + UNIT * q), ("rb", part[0, q]), ("rb", got[1, 0, q]), ("rb", got[-1, 0, q])])
        for q in range(4)
    ]
    p.final_txt = []
    for o, one, two, at in HALVES:
        n = REDUCE_XY
        base = {}
        for u in RING4:
            far, last = {}, {}
            for s, w in SIDES:
                q = 0 if s == 1 else 1
                far[s, q] = p.reduce(two + w, UNIT, [("gt", at(u, 2) + o + UNIT * q)])
            for s, w in SIDES:
                for q in range(0, 2, n // UNIT):
                    pieces = [[("gt", at(u, s) + o + UNIT * e)] + ([("rb", far[s, e])] if (s, e) in far else [])
                              for e in range(q, q + n // UNIT)]
                    row = p.reduce(two + w, n, *pieces)
                    for k in range(n // UNIT):
                        last[s, q + k] = row + UNIT * k
            for q in (0, 1):
                base[u, q] = [("gt", at(u, 0) + o + UNIT * q), ("rb", last[1, q]), ("rb", last[-1, q])]
        far, last = {}, {}
        for s, w in SIDES:
            q = 0 if s == 1 else 1
            far[s, q] = p.reduce(one + w, UNIT, base[2, q])
        for s, w in SIDES:
            for q in range(0, 2, n // UNIT):
                pieces = [base[s, e] + ([("rb", far[s, e])] if (s, e) in far else []) for e in range(q, q + n // UNIT)]
                row = p.reduce(one + w, n, *pieces)
                for k in range(n // UNIT):
                    last[s, q + k] = row + UNIT * k
        for q in (0, 1):
            p.final_txt.append((o + UNIT * q, base[0, q] + [("rb", last[1, q]), ("rb", last[-1, q])]))
    return p


PLAN = make_plan()

ORDER = (
    15, 19, 88, 8, 68, 78, 58, 0, 56, 57, 14, 18, 69, 16, 20, 9, 59, 79, 89, 17, 21, 10, 1, 2, 23, 27, 80, 90, 22,
    26, 83, 93, 53, 54, 60, 71, 24, 28, 63, 73, 25, 29, 55, 52, 81, 91, 11, 70, 3, 61, 4, 31, 35, 30, 34, 49, 50,
    82, 92, 74, 64, 32, 36, 12, 72, 62, 33, 85, 37, 95, 48, 51, 1033, 5, 6, 84, 94, 39, 41, 65, 76, 1023, 86, 96,
    38, 40, 45, 46, 13, 75, 66, 1032, 1022, 87, 97, 47, 44, 7, 67, 77, 1013, 1012, 1220, 43, 42, 1011, 1110, 1031,
    1021, 1210, 1003, 1002, 1030, 1010, 1020, 1200, 1001, 1100, 1000, 1201, 175, 174, 155, 154, 1101, 99, 98, 100,
    167, 166, 147, 101, 150, 1211, 171, 170, 143, 146, 116, 1111, 114, 102, 103, 104, 117, 115, 142, 151, 163, 105,
    162, 1120, 177, 176, 157, 125, 120, 156, 1121, 106, 107, 124, 108, 121, 109, 1221, 168, 169, 122, 149, 118, 152,
    1130, 123, 1131, 119, 173, 110, 172, 153, 148, 112, 133, 128, 111, 113, 1230, 132, 129, 159, 179, 158, 178,
    1231, 130, 126, 165, 145, 164, 144, 131, 127, 141, 136, 140, 137, 161, 160, 181, 180, 138, 134, 139, 135,
)


def unit_rows(v):
    v = v.astype(F32)
    inv = lax.rsqrt(jnp.sum(v * v, axis=1, keepdims=True) + 1e-6)
    return v * inv, inv


def kernel(ie_ref, te_ref, ii_ref, ti_ref, oi_ref, ot_ref,
           ie, te, ids, img, txt, coef, gi, gt, sb, rb, iid, tid, icol, ssem, rsem, isem):
    blk, rep, sub = lax.axis_index("blk"), lax.axis_index("rep"), lax.axis_index("sub")
    where = {
        "x+": {"sub": lax.rem(sub + 1, 4)}, "x-": {"sub": lax.rem(sub + 3, 4)},
        "y+": {"blk": lax.rem(blk + 2, 8)}, "y-": {"blk": lax.rem(blk + 6, 8)},
        "z+": {"rep": lax.rem(rep + 1, 8)}, "z-": {"rep": lax.rem(rep + 7, 8)},
        "c": {"blk": blk + 1 - 2 * lax.rem(blk, 2)},
    }
    barrier = pltpu.get_barrier_semaphore()
    for way in where.values():
        pl.semaphore_signal(barrier, inc=1, device_id=way, device_id_type=MESH)
    loads = [
        pltpu.make_async_copy(src, dst, isem.at[k])
        for k, (src, dst) in enumerate(((ie_ref, ie), (te_ref, te), (ii_ref, ids.at[0]), (ti_ref, ids.at[1])))
    ]
    for load in loads:
        load.start()
    for load in loads:
        load.wait()
    img[pl.ds(img_row(0, 0), ROWS), :] = unit_rows(ie[...])[0].astype(BF16)
    txt[pl.ds(txt_row(0, 0), ROWS), :] = unit_rows(te[...])[0].astype(BF16)
    for k, ref, row in ((0, iid, iid_row(0)), (1, tid, tid_row(0, 0))):
        ref[row] = jnp.concatenate([ids[k], ids[k]], axis=1)
    pl.semaphore_wait(barrier, len(where))

    bufs = {"img": img, "txt": txt, "gi": gi, "gt": gt, "sb": sb, "rb": rb, "iid": iid, "tid": tid}

    def copy(index):
        way, src, dst, _ = PLAN.msgs[index]
        return pltpu.make_async_remote_copy(
            src_ref=bufs[src[0]].at[pl.ds(src[1], src[2])],
            dst_ref=bufs[dst[0]].at[pl.ds(dst[1], dst[2])],
            send_sem=ssem.at[index], recv_sem=rsem.at[index],
            device_id=where[way], device_id_type=MESH,
        )

    here, sent = set(), []

    def need(buf, row, n):
        for r in range(row, row + n):
            name = PLAN.origin.get((buf, r))
            if name is not None and name not in here:
                here.add(name)
                copy(name).wait_recv()

    def total(n, terms):
        acc = None
        for buf, row in terms:
            need(buf, row, n)
            v = bufs[buf][pl.ds(row, n), :].astype(F32)
            acc = v if acc is None else acc + v
        return acc

    def send(name):
        _, src, _, pieces = PLAN.msgs[name]
        if pieces is None:
            need(*src)
        else:
            n = src[2] // len(pieces)
            for k, terms in enumerate(pieces):
                sb[pl.ds(src[1] + n * k, n), :] = total(n, terms).astype(BF16)
        copy(name).start()
        sent.append(name)

    lane = lax.broadcasted_iota(jnp.int32, (1, 128), 1)
    ready = set()

    def columns(row, n):
        for p in range(row // 128, (row + n) // 128):
            if p not in ready:
                ready.add(p)
                need("iid", 2 * p, 2)
                both_ids = jnp.where(lane < 64, iid[2 * p], iid[2 * p + 1])
                icol[pl.ds(128 * p, 128), :] = jnp.transpose(jnp.broadcast_to(both_ids, (128, 128)))

    def tile(i, m, t, n):
        need("img", i, m)
        need("txt", t, n)
        columns(i, m)
        keys = []
        for b in range(t // 64, (t + n) // 64, 2):
            r0, r1 = tid_row(*T_ORDER[b]), tid_row(*T_ORDER[b + 1])
            need("tid", r0, 1)
            need("tid", r1, 1)
            keys.append(jnp.where(lane < 64, tid[r0], tid[r1]))
        z = lax.dot_general(img[pl.ds(i, m), :], txt[pl.ds(t, n), :],
                            (((1,), (1,)), ((), ())), preferred_element_type=F32)
        sig = jax.nn.sigmoid(SCALE * z + BIAS)
        rows = icol[pl.ds(i, m), :]
        same = jnp.concatenate([(rows == k).astype(F32) for k in keys], axis=1)
        coef[pl.ds(i, m), pl.ds(t, n)] = (SCALE * (sig - same)).astype(BF16)

    def gradient(ref, row, n, part, g):
        rows = pl.ds(row, n)
        ref[rows, :] = ref[rows, :] + g if part else g

    for step in ORDER:
        if step < 1000:
            send(step)
            continue
        c, part = step // 10 % 10, step % 10
        if step < 1100:
            tile(*IMG_CHUNKS[c], *TXT_CHUNKS[part])
        elif step < 1200:
            (i, m), first = IMG_CHUNKS[c], TXT_CHUNKS[0][1]
            ks = pl.ds(0, first) if part else pl.ds(first, 1024 - first)
            gradient(gi, i, m, part, jnp.dot(coef[pl.ds(i, m), ks], txt[ks, :], preferred_element_type=F32))
        else:
            (t, n), first = TXT_CHUNKS[c], IMG_CHUNKS[0][1]
            ks = pl.ds(0, first) if part else pl.ds(first, 1024 - first)
            gradient(gt, t, n, part, lax.dot_general(coef[ks, pl.ds(t, n)], img[ks, :], (((0,), (0,)), ((), ())),
                                                     preferred_element_type=F32))
    for pieces, out in ((PLAN.final_img, oi_ref), (PLAN.final_txt, ot_ref)):
        for row, terms in pieces:
            out[pl.ds(row, UNIT), :] = total(UNIT, terms)
    n_msgs = len(PLAN.msgs)
    assert len(sent) == n_msgs and len(here) == n_msgs
    for name in sent:
        copy(name).wait_send()


def project(ie_ref, te_ref, gi_ref, gt_ref, oi_ref, ot_ref):
    for embed, grad, out in ((ie_ref, gi_ref, oi_ref), (te_ref, gt_ref, ot_ref)):
        unit, inv = unit_rows(embed[...])
        g = grad[...]
        along = jnp.sum(unit * g, axis=1, keepdims=True)
        out[...] = (g - unit * along) * inv


def body(image_embed, text_embed, image_ids, text_ids):
    vmem, hbm = pl.BlockSpec(memory_space=pltpu.VMEM), pl.BlockSpec(memory_space=pltpu.HBM)
    n = len(PLAN.msgs)
    out = jax.ShapeDtypeStruct((ROWS, D), F32)
    sums = pl.pallas_call(
        kernel,
        name="pairs",
        out_shape=(out, out),
        in_specs=[hbm] * 4,
        out_specs=(vmem, vmem),
        scratch_shapes=[
            pltpu.VMEM((ROWS, D), BF16),
            pltpu.VMEM((ROWS, D), BF16),
            pltpu.VMEM((2, 1, ROWS), jnp.int32),
            pltpu.VMEM((1024, D), BF16),
            pltpu.VMEM((1024, D), BF16),
            pltpu.VMEM((1024, 1024), BF16),
            pltpu.VMEM((1024, D), F32),
            pltpu.VMEM((1024, D), F32),
            pltpu.VMEM((PLAN.rows["sb"], D), BF16),
            pltpu.VMEM((PLAN.rows["rb"], D), BF16),
            pltpu.VMEM((16, 1, 128), jnp.int32),
            pltpu.VMEM((16, 1, 128), jnp.int32),
            pltpu.VMEM((1024, 128), jnp.int32),
            pltpu.SemaphoreType.DMA((n,)),
            pltpu.SemaphoreType.DMA((n,)),
            pltpu.SemaphoreType.DMA((4,)),
        ],
        compiler_params=pltpu.CompilerParams(
            collective_id=0, has_side_effects=True, vmem_limit_bytes=48 * 1024 * 1024
        ),
    )(*(pltpu.with_memory_space_constraint(a, pltpu.HBM)
        for a in (image_embed, text_embed, image_ids.reshape(1, ROWS), text_ids.reshape(1, ROWS))))
    return pl.pallas_call(
        project,
        name="project",
        out_shape=(out, out),
        in_specs=[vmem] * 4,
        out_specs=(vmem, vmem),
        compiler_params=pltpu.CompilerParams(vmem_limit_bytes=4 * 1024 * 1024),
    )(image_embed, text_embed, *sums)


def solution(mesh):
    rows = P(("blk", "rep", "sub"), None)
    flat = P(("blk", "rep", "sub"))
    return jax.shard_map(
        body, mesh=mesh, in_specs=(rows, rows, flat, flat), out_specs=(rows, rows), check_vma=False
    )
```

```python
import jax
import jax.numpy as jnp
from jax import lax
from jax.experimental import pallas as pl
from jax.experimental.pallas import tpu as pltpu
from jax.sharding import PartitionSpec as P

SCALE = 30.0
BIAS = -3.0
ROWS = 64
D = 1152
UNIT = 16
GATHER_XY, REDUCE_XY = 32, 32
PARTS_Z = {1: ((0, 16), (16, 16), (32, 16), (48, 16)), -1: ((48, 16), (32, 16), (16, 16), (0, 16))}
IMG_CHUNKS = ((0, 256), (256, 256), (512, 256), (768, 256))
TXT_CHUNKS = ((0, 256), (256, 256), (512, 256), (768, 256))
TERMS = ((512, 512), (0, 512))
MESH = pl.DeviceIdType.MESH
F32 = jnp.float32
BF16 = jnp.bfloat16

Z_ORDER = (4, 3, -3, 2, -2, 1, -1, 0)
T_ORDER = (
    (2, 2), (1, 2), (2, 1), (-1, 2), (2, -1), (0, 2), (2, 0), (1, 1),
    (-1, 1), (1, -1), (-1, -1), (0, 1), (1, 0), (0, -1), (-1, 0), (0, 0),
)
RING4 = (0, 1, -1, 2)


def near4(d):
    return (d + 1) % 4 - 1


def near8(d):
    return (d + 3) % 8 - 3


def img_row(lane, dz):
    return Z_ORDER.index(near8(dz)) * 128 + lane * 64


def txt_row(dx, dy):
    return T_ORDER.index((near4(dx), near4(dy))) * 64


def tid_row(dx, dy):
    return RING4.index(near4(dy)) * 4 + RING4.index(near4(dx))


def iid_row(dz):
    return Z_ORDER.index(near8(dz)) * 2


class Plan:
    def __init__(self):
        self.msgs = []
        self.origin = {}
        self.rows = {"sb": 0, "rb": 0}

    def add(self, way, src, dst, pieces=None):
        buf, row, n = dst
        for r in range(row, row + n):
            assert (buf, r) not in self.origin
            self.origin[buf, r] = len(self.msgs)
        self.msgs.append((way, src, dst, pieces))

    def room(self, buf, n):
        row = self.rows[buf]
        self.rows[buf] += n
        return row

    def reduce(self, way, n, *pieces):
        src, dst = self.room("sb", n), self.room("rb", n)
        self.add(way, ("sb", src, n), ("rb", dst, n), pieces)
        return dst


SIDES = ((1, "+"), (-1, "-"))
HALVES = ((0, "x", "y", lambda u, v: txt_row(u, v)), (32, "y", "x", lambda u, v: txt_row(v, u)))


def make_plan():
    p = Plan()
    p.add("c", ("iid", iid_row(0), 1), ("iid", iid_row(0) + 1, 1))
    for k in range(4):
        p.add("z+", ("iid", iid_row(-k), 2), ("iid", iid_row(-k - 1), 2))
        if k < 3:
            p.add("z-", ("iid", iid_row(k), 2), ("iid", iid_row(k + 1), 2))
    p.add("x+", ("tid", tid_row(0, 0), 1), ("tid", tid_row(-1, 0), 1))
    p.add("x-", ("tid", tid_row(0, 0), 1), ("tid", tid_row(1, 0), 1))
    p.add("x+", ("tid", tid_row(-1, 0), 1), ("tid", tid_row(2, 0), 1))
    p.add("y+", ("tid", tid_row(0, 0), 4), ("tid", tid_row(0, -1), 4))
    p.add("y-", ("tid", tid_row(0, 0), 4), ("tid", tid_row(0, 1), 4))
    p.add("y+", ("tid", tid_row(0, -1), 4), ("tid", tid_row(0, 2), 4))
    for k in range(4):
        for s, w in SIDES:
            for q, n in PARTS_Z[s]:
                if k < 3 or (q < 32) == (s == 1):
                    p.add("z" + w, ("img", img_row(0, -s * k) + q, n), ("img", img_row(0, -s * (k + 1)) + q, n))
    for dz in Z_ORDER:
        for h in (0, 1):
            p.add("c", ("img", img_row(0, dz) + 32 * h, 32), ("img", img_row(1, dz) + 32 * h, 32))
    for o, one, two, at in HALVES:
        n = GATHER_XY
        for s, w in SIDES:
            for q in range(0, 32, n):
                p.add(one + w, ("txt", at(0, 0) + o + q, n), ("txt", at(-s, 0) + o + q, n))
                for u in RING4:
                    p.add(two + w, ("txt", at(u, 0) + o + q, n), ("txt", at(u, -s) + o + q, n))
            e = o if s == 1 else o + UNIT
            p.add(one + w, ("txt", at(-s, 0) + e, UNIT), ("txt", at(2, 0) + e, UNIT))
            for u in RING4:
                p.add(two + w, ("txt", at(u, -s) + e, UNIT), ("txt", at(u, 2) + e, UNIT))
    part = {}
    for dz in Z_ORDER:
        for h in (0, 1):
            row = p.reduce("c", 32, [("gi", img_row(1, dz) + 32 * h)])
            part[dz, 2 * h], part[dz, 2 * h + 1] = row, row + UNIT
    got = {}
    for j in (4, 3, 2, 1):
        for s, w in SIDES:
            for q, n in PARTS_Z[s]:
                if j == 4 and (q < 32) != (s == 1):
                    continue
                dz, pieces = near8(s * j), []
                for e in range(q // UNIT, (q + n) // UNIT):
                    terms = [("gi", img_row(0, dz) + UNIT * e), ("rb", part[dz, e])]
                    if (s, j, e) in got:
                        terms.append(("rb", got[s, j, e]))
                    pieces.append(terms)
                row = p.reduce("z" + w, n, *pieces)
                for k in range(n // UNIT):
                    got[s, j - 1, q // UNIT + k] = row + UNIT * k
    p.final_img = [
        (UNIT * q, [("gi", img_row(0, 0) + UNIT * q), ("rb", part[0, q]), ("rb", got[1, 0, q]), ("rb", got[-1, 0, q])])
        for q in range(4)
    ]
    p.final_txt = []
    for o, one, two, at in HALVES:
        n = REDUCE_XY
        base = {}
        for u in RING4:
            far, last = {}, {}
            for s, w in SIDES:
                q = 0 if s == 1 else 1
                far[s, q] = p.reduce(two + w, UNIT, [("gt", at(u, 2) + o + UNIT * q)])
            for s, w in SIDES:
                for q in range(0, 2, n // UNIT):
                    pieces = [[("gt", at(u, s) + o + UNIT * e)] + ([("rb", far[s, e])] if (s, e) in far else [])
                              for e in range(q, q + n // UNIT)]
                    row = p.reduce(two + w, n, *pieces)
                    for k in range(n // UNIT):
                        last[s, q + k] = row + UNIT * k
            for q in (0, 1):
                base[u, q] = [("gt", at(u, 0) + o + UNIT * q), ("rb", last[1, q]), ("rb", last[-1, q])]
        far, last = {}, {}
        for s, w in SIDES:
            q = 0 if s == 1 else 1
            far[s, q] = p.reduce(one + w, UNIT, base[2, q])
        for s, w in SIDES:
            for q in range(0, 2, n // UNIT):
                pieces = [base[s, e] + ([("rb", far[s, e])] if (s, e) in far else []) for e in range(q, q + n // UNIT)]
                row = p.reduce(one + w, n, *pieces)
                for k in range(n // UNIT):
                    last[s, q + k] = row + UNIT * k
        for q in (0, 1):
            p.final_txt.append((o + UNIT * q, base[0, q] + [("rb", last[1, q]), ("rb", last[-1, q])]))
    return p


PLAN = make_plan()
KIND = {"iid": "iid", "tid": "iid", "img": "img", "txt": "img", "sb": "sb"}

ORDER = (
    78, 58, 88, 68, 15, 18, 0, 57, 56, 16, 19, 59, 8, 69, 9, 79, 89, 14, 20, 1, 21, 17, 2, 23, 26, 83, 63, 93, 73,
    24, 27, 53, 60, 10, 70, 90, 80, 22, 28, 54, 3, 29, 52, 25, 61, 55, 71, 91, 81, 4, 31, 34, 11, 72, 92, 32, 35,
    82, 62, 49, 30, 36, 50, 5, 12, 95, 85, 65, 75, 37, 48, 51, 33, 6, 94, 84, 64, 74, 39, 40, 1023, 41, 13, 66, 45,
    76, 86, 96, 1033, 1230, 38, 46, 77, 97, 87, 67, 1032, 7, 1022, 44, 47, 1120, 1220, 1130, 1012, 1013, 43, 1110,
    1011, 42, 1021, 1031, 1020, 1030, 1200, 1000, 1010, 1201, 175, 174, 154, 155, 1003, 167, 166, 146, 147, 1001,
    1002, 1100, 150, 151, 1101, 98, 99, 100, 101, 1111, 105, 104, 102, 103, 114, 117, 177, 176, 156, 115, 116, 1210,
    1211, 157, 120, 170, 171, 142, 124, 1121, 106, 121, 125, 163, 107, 143, 168, 109, 148, 108, 118, 123, 1221, 169,
    149, 152, 119, 122, 162, 1231, 128, 132, 173, 172, 179, 178, 129, 133, 153, 1131, 110, 144, 159, 126, 131, 158,
    111, 113, 112, 165, 127, 145, 130, 164, 136, 140, 137, 141, 180, 181, 134, 139, 160, 161, 135, 138,
)


def unit_rows(v):
    v = v.astype(F32)
    inv = lax.rsqrt(jnp.sum(v * v, axis=1, keepdims=True) + 1e-6)
    return v * inv, inv


def kernel(ie_ref, te_ref, ii_ref, ti_ref, oi_ref, ot_ref,
           ie, te, ids, img, txt, coef, gi, gt, sb, rb, iid, tid, icol, ssem, rsem, isem):
    blk, rep, sub = lax.axis_index("blk"), lax.axis_index("rep"), lax.axis_index("sub")
    where = {
        "x+": {"sub": lax.rem(sub + 1, 4)}, "x-": {"sub": lax.rem(sub + 3, 4)},
        "y+": {"blk": lax.rem(blk + 2, 8)}, "y-": {"blk": lax.rem(blk + 6, 8)},
        "z+": {"rep": lax.rem(rep + 1, 8)}, "z-": {"rep": lax.rem(rep + 7, 8)},
        "c": {"blk": blk + 1 - 2 * lax.rem(blk, 2)},
    }
    barrier = pltpu.get_barrier_semaphore()
    for way in where.values():
        pl.semaphore_signal(barrier, inc=1, device_id=way, device_id_type=MESH)
    loads = [
        pltpu.make_async_copy(src, dst, isem.at[k])
        for k, (src, dst) in enumerate(((ie_ref, ie), (te_ref, te), (ii_ref, ids.at[0]), (ti_ref, ids.at[1])))
    ]
    for load in loads:
        load.start()
    for load in loads:
        load.wait()
    img[pl.ds(img_row(0, 0), ROWS), :] = unit_rows(ie[...])[0].astype(BF16)
    txt[pl.ds(txt_row(0, 0), ROWS), :] = unit_rows(te[...])[0].astype(BF16)
    for k, ref, row in ((0, iid, iid_row(0)), (1, tid, tid_row(0, 0))):
        ref[row] = jnp.concatenate([ids[k], ids[k]], axis=1)
    pl.semaphore_wait(barrier, len(where))

    bufs = {"img": img, "txt": txt, "gi": gi, "gt": gt, "sb": sb, "rb": rb, "iid": iid, "tid": tid}

    def copy(index):
        way, src, dst, _ = PLAN.msgs[index]
        return pltpu.make_async_remote_copy(
            src_ref=bufs[src[0]].at[pl.ds(src[1], src[2])],
            dst_ref=bufs[dst[0]].at[pl.ds(dst[1], dst[2])],
            send_sem=ssem.at[("iid", "img", "sb").index(KIND[src[0]])], recv_sem=rsem.at[index],
            device_id=where[way], device_id_type=MESH,
        )

    here, sent = set(), []

    def need(buf, row, n):
        for r in range(row, row + n):
            name = PLAN.origin.get((buf, r))
            if name is not None and name not in here:
                here.add(name)
                copy(name).wait_recv()

    def total(n, terms):
        acc = None
        for buf, row in terms:
            need(buf, row, n)
            v = bufs[buf][pl.ds(row, n), :].astype(F32)
            acc = v if acc is None else acc + v
        return acc

    def send(name):
        _, src, _, pieces = PLAN.msgs[name]
        if pieces is None:
            need(*src)
        else:
            n = src[2] // len(pieces)
            for k, terms in enumerate(pieces):
                sb[pl.ds(src[1] + n * k, n), :] = total(n, terms).astype(BF16)
        copy(name).start()
        sent.append(name)

    lane = lax.broadcasted_iota(jnp.int32, (1, 128), 1)
    ready = set()

    def columns(row, n):
        for p in range(row // 128, (row + n) // 128):
            if p not in ready:
                ready.add(p)
                need("iid", 2 * p, 2)
                both_ids = jnp.where(lane < 64, iid[2 * p], iid[2 * p + 1])
                icol[pl.ds(128 * p, 128), :] = jnp.transpose(jnp.broadcast_to(both_ids, (128, 128)))

    def tile(i, m, t, n):
        need("img", i, m)
        need("txt", t, n)
        columns(i, m)
        keys = []
        for b in range(t // 64, (t + n) // 64, 2):
            r0, r1 = tid_row(*T_ORDER[b]), tid_row(*T_ORDER[b + 1])
            need("tid", r0, 1)
            need("tid", r1, 1)
            keys.append(jnp.where(lane < 64, tid[r0], tid[r1]))
        z = lax.dot_general(img[pl.ds(i, m), :], txt[pl.ds(t, n), :],
                            (((1,), (1,)), ((), ())), preferred_element_type=F32)
        sig = jax.nn.sigmoid(SCALE * z + BIAS)
        rows = icol[pl.ds(i, m), :]
        same = jnp.concatenate([(rows == k).astype(F32) for k in keys], axis=1)
        coef[pl.ds(i, m), pl.ds(t, n)] = (SCALE * (sig - same)).astype(BF16)

    def gradient(ref, row, n, part, g):
        rows = pl.ds(row, n)
        ref[rows, :] = ref[rows, :] + g if part else g

    for step in ORDER:
        if step < 1000:
            send(step)
            continue
        c, part = step // 10 % 10, step % 10
        if step < 1100:
            tile(*IMG_CHUNKS[c], *TXT_CHUNKS[part])
        elif step < 1200:
            (i, m), ks = IMG_CHUNKS[c], pl.ds(*TERMS[part])
            gradient(gi, i, m, part, jnp.dot(coef[pl.ds(i, m), ks], txt[ks, :], preferred_element_type=F32))
        else:
            (t, n), ks = TXT_CHUNKS[c], pl.ds(*TERMS[part])
            gradient(gt, t, n, part, lax.dot_general(coef[ks, pl.ds(t, n)], img[ks, :], (((0,), (0,)), ((), ())),
                                                     preferred_element_type=F32))
    for pieces, out in ((PLAN.final_img, oi_ref), (PLAN.final_txt, ot_ref)):
        for row, terms in pieces:
            out[pl.ds(row, UNIT), :] = total(UNIT, terms)
    n_msgs = len(PLAN.msgs)
    assert len(sent) == n_msgs and len(here) == n_msgs
    for kind, ref in (("iid", tid), ("img", sb), ("sb", sb)):
        n = sum(src[2] for _, src, _, _ in PLAN.msgs if KIND[src[0]] == kind)
        k = ("iid", "img", "sb").index(kind)
        pltpu.make_async_copy(ref.at[pl.ds(0, n)], ref.at[pl.ds(0, n)], ssem.at[k]).wait()


def project(ie_ref, te_ref, gi_ref, gt_ref, oi_ref, ot_ref):
    for embed, grad, out in ((ie_ref, gi_ref, oi_ref), (te_ref, gt_ref, ot_ref)):
        unit, inv = unit_rows(embed[...])
        g = grad[...]
        along = jnp.sum(unit * g, axis=1, keepdims=True)
        out[...] = (g - unit * along) * inv


def body(image_embed, text_embed, image_ids, text_ids):
    vmem, hbm = pl.BlockSpec(memory_space=pltpu.VMEM), pl.BlockSpec(memory_space=pltpu.HBM)
    n = len(PLAN.msgs)
    out = jax.ShapeDtypeStruct((ROWS, D), F32)
    sums = pl.pallas_call(
        kernel,
        name="pairs",
        out_shape=(out, out),
        in_specs=[hbm] * 4,
        out_specs=(vmem, vmem),
        scratch_shapes=[
            pltpu.VMEM((ROWS, D), BF16),
            pltpu.VMEM((ROWS, D), BF16),
            pltpu.VMEM((2, 1, ROWS), jnp.int32),
            pltpu.VMEM((1024, D), BF16),
            pltpu.VMEM((1024, D), BF16),
            pltpu.VMEM((1024, 1024), BF16),
            pltpu.VMEM((1024, D), F32),
            pltpu.VMEM((1024, D), F32),
            pltpu.VMEM((PLAN.rows["sb"], D), BF16),
            pltpu.VMEM((PLAN.rows["rb"], D), BF16),
            pltpu.VMEM((16, 1, 128), jnp.int32),
            pltpu.VMEM((32, 1, 128), jnp.int32),
            pltpu.VMEM((1024, 128), jnp.int32),
            pltpu.SemaphoreType.DMA((3,)),
            pltpu.SemaphoreType.DMA((n,)),
            pltpu.SemaphoreType.DMA((4,)),
        ],
        compiler_params=pltpu.CompilerParams(
            collective_id=0, has_side_effects=True, vmem_limit_bytes=48 * 1024 * 1024
        ),
    )(*(pltpu.with_memory_space_constraint(a, pltpu.HBM)
        for a in (image_embed, text_embed, image_ids.reshape(1, ROWS), text_ids.reshape(1, ROWS))))
    return pl.pallas_call(
        project,
        name="project",
        out_shape=(out, out),
        in_specs=[vmem] * 4,
        out_specs=(vmem, vmem),
        compiler_params=pltpu.CompilerParams(vmem_limit_bytes=4 * 1024 * 1024),
    )(image_embed, text_embed, *sums)


def solution(mesh):
    rows = P(("blk", "rep", "sub"), None)
    flat = P(("blk", "rep", "sub"))
    return jax.shard_map(
        body, mesh=mesh, in_specs=(rows, rows, flat, flat), out_specs=(rows, rows), check_vma=False
    )
```

```python
import jax
import jax.numpy as jnp
from jax import lax
from jax.experimental import pallas as pl
from jax.experimental.pallas import tpu as pltpu
from jax.sharding import PartitionSpec as P

SCALE = 30.0
BIAS = -3.0
ROWS = 64
D = 1152
UNIT = 16
GATHER_XY, REDUCE_XY = 32, 32
PARTS_Z = {1: ((0, 16), (16, 16), (32, 16), (48, 16)), -1: ((48, 16), (32, 16), (16, 16), (0, 16))}
IMG_CHUNKS = ((0, 256), (256, 256), (512, 256), (768, 256))
TXT_CHUNKS = ((0, 256), (256, 256), (512, 256), (768, 256))
TERMS = ((512, 512), (0, 512))
MESH = pl.DeviceIdType.MESH
F32 = jnp.float32
BF16 = jnp.bfloat16

Z_ORDER = (4, 3, -3, 2, -2, 1, -1, 0)
T_ORDER = (
    (2, 2), (1, 2), (2, 1), (-1, 2), (2, -1), (0, 2), (2, 0), (1, 1),
    (-1, 1), (1, -1), (-1, -1), (0, 1), (1, 0), (0, -1), (-1, 0), (0, 0),
)
RING4 = (0, 1, -1, 2)


def near4(d):
    return (d + 1) % 4 - 1


def near8(d):
    return (d + 3) % 8 - 3


def img_row(lane, dz):
    return Z_ORDER.index(near8(dz)) * 128 + lane * 64


def txt_row(dx, dy):
    return T_ORDER.index((near4(dx), near4(dy))) * 64


def tid_row(dx, dy):
    return RING4.index(near4(dy)) * 4 + RING4.index(near4(dx))


def iid_row(dz):
    return Z_ORDER.index(near8(dz)) * 2


class Plan:
    def __init__(self):
        self.msgs = []
        self.origin = {}
        self.rows = {"sb": 0, "rb": 0}

    def add(self, way, src, dst, pieces=None):
        buf, row, n = dst
        for r in range(row, row + n):
            assert (buf, r) not in self.origin
            self.origin[buf, r] = len(self.msgs)
        self.msgs.append((way, src, dst, pieces))

    def room(self, buf, n):
        row = self.rows[buf]
        self.rows[buf] += n
        return row

    def reduce(self, way, n, *pieces):
        src, dst = self.room("sb", n), self.room("rb", n)
        self.add(way, ("sb", src, n), ("rb", dst, n), pieces)
        return dst


SIDES = ((1, "+"), (-1, "-"))
HALVES = ((0, "x", "y", lambda u, v: txt_row(u, v)), (32, "y", "x", lambda u, v: txt_row(v, u)))


def make_plan():
    p = Plan()
    p.add("c", ("iid", iid_row(0), 1), ("iid", iid_row(0) + 1, 1))
    for k in range(4):
        p.add("z+", ("iid", iid_row(-k), 2), ("iid", iid_row(-k - 1), 2))
        if k < 3:
            p.add("z-", ("iid", iid_row(k), 2), ("iid", iid_row(k + 1), 2))
    p.add("x+", ("tid", tid_row(0, 0), 1), ("tid", tid_row(-1, 0), 1))
    p.add("x-", ("tid", tid_row(0, 0), 1), ("tid", tid_row(1, 0), 1))
    p.add("x+", ("tid", tid_row(-1, 0), 1), ("tid", tid_row(2, 0), 1))
    p.add("y+", ("tid", tid_row(0, 0), 4), ("tid", tid_row(0, -1), 4))
    p.add("y-", ("tid", tid_row(0, 0), 4), ("tid", tid_row(0, 1), 4))
    p.add("y+", ("tid", tid_row(0, -1), 4), ("tid", tid_row(0, 2), 4))
    for k in range(4):
        for s, w in SIDES:
            for q, n in PARTS_Z[s]:
                if k < 3 or (q < 32) == (s == 1):
                    p.add("z" + w, ("img", img_row(0, -s * k) + q, n), ("img", img_row(0, -s * (k + 1)) + q, n))
    for dz in Z_ORDER:
        for h in (0, 1):
            p.add("c", ("img", img_row(0, dz) + 32 * h, 32), ("img", img_row(1, dz) + 32 * h, 32))
    for o, one, two, at in HALVES:
        n = GATHER_XY
        for s, w in SIDES:
            for q in range(0, 32, n):
                p.add(one + w, ("txt", at(0, 0) + o + q, n), ("txt", at(-s, 0) + o + q, n))
                for u in RING4:
                    p.add(two + w, ("txt", at(u, 0) + o + q, n), ("txt", at(u, -s) + o + q, n))
            e = o if s == 1 else o + UNIT
            p.add(one + w, ("txt", at(-s, 0) + e, UNIT), ("txt", at(2, 0) + e, UNIT))
            for u in RING4:
                p.add(two + w, ("txt", at(u, -s) + e, UNIT), ("txt", at(u, 2) + e, UNIT))
    part = {}
    for dz in Z_ORDER:
        for h in (0, 1):
            row = p.reduce("c", 32, [("gi", img_row(1, dz) + 32 * h)])
            part[dz, 2 * h], part[dz, 2 * h + 1] = row, row + UNIT
    got = {}
    for j in (4, 3, 2, 1):
        for s, w in SIDES:
            for q, n in PARTS_Z[s]:
                if j == 4 and (q < 32) != (s == 1):
                    continue
                dz, pieces = near8(s * j), []
                for e in range(q // UNIT, (q + n) // UNIT):
                    terms = [("gi", img_row(0, dz) + UNIT * e), ("rb", part[dz, e])]
                    if (s, j, e) in got:
                        terms.append(("rb", got[s, j, e]))
                    pieces.append(terms)
                row = p.reduce("z" + w, n, *pieces)
                for k in range(n // UNIT):
                    got[s, j - 1, q // UNIT + k] = row + UNIT * k
    p.final_img = [
        (UNIT * q, [("gi", img_row(0, 0) + UNIT * q), ("rb", part[0, q]), ("rb", got[1, 0, q]), ("rb", got[-1, 0, q])])
        for q in range(4)
    ]
    p.final_txt = []
    for o, one, two, at in HALVES:
        n = REDUCE_XY
        base = {}
        for u in RING4:
            far, last = {}, {}
            for s, w in SIDES:
                q = 0 if s == 1 else 1
                far[s, q] = p.reduce(two + w, UNIT, [("gt", at(u, 2) + o + UNIT * q)])
            for s, w in SIDES:
                for q in range(0, 2, n // UNIT):
                    pieces = [[("gt", at(u, s) + o + UNIT * e)] + ([("rb", far[s, e])] if (s, e) in far else [])
                              for e in range(q, q + n // UNIT)]
                    row = p.reduce(two + w, n, *pieces)
                    for k in range(n // UNIT):
                        last[s, q + k] = row + UNIT * k
            for q in (0, 1):
                base[u, q] = [("gt", at(u, 0) + o + UNIT * q), ("rb", last[1, q]), ("rb", last[-1, q])]
        far, last = {}, {}
        for s, w in SIDES:
            q = 0 if s == 1 else 1
            far[s, q] = p.reduce(one + w, UNIT, base[2, q])
        for s, w in SIDES:
            for q in range(0, 2, n // UNIT):
                pieces = [base[s, e] + ([("rb", far[s, e])] if (s, e) in far else []) for e in range(q, q + n // UNIT)]
                row = p.reduce(one + w, n, *pieces)
                for k in range(n // UNIT):
                    last[s, q + k] = row + UNIT * k
        for q in (0, 1):
            p.final_txt.append((o + UNIT * q, base[0, q] + [("rb", last[1, q]), ("rb", last[-1, q])]))
    return p


PLAN = make_plan()
KIND = {"iid": "iid", "tid": "iid", "img": "img", "txt": "img", "sb": "sb"}

ORDER = (
    78, 58, 88, 68, 15, 18, 0, 57, 56, 16, 19, 59, 8, 69, 9, 79, 89, 14, 20, 1, 21, 17, 2, 23, 26, 83, 63, 93, 73,
    24, 27, 53, 60, 10, 70, 90, 80, 22, 28, 54, 3, 29, 52, 25, 61, 55, 71, 91, 81, 4, 31, 34, 11, 72, 92, 32, 35,
    82, 62, 49, 30, 36, 50, 5, 12, 95, 85, 65, 75, 37, 48, 51, 33, 6, 94, 84, 64, 74, 39, 40, 1023, 41, 13, 66, 45,
    76, 86, 96, 1033, 1230, 38, 46, 77, 97, 87, 67, 1032, 7, 1022, 44, 47, 1120, 1220, 1130, 1012, 1013, 43, 1110,
    1011, 42, 1021, 1031, 1020, 1030, 1200, 1000, 1010, 1201, 175, 174, 154, 155, 1003, 167, 166, 146, 147, 1001,
    1002, 1100, 150, 151, 1101, 98, 99, 100, 101, 1111, 105, 104, 102, 103, 114, 117, 177, 176, 156, 115, 116, 1210,
    1211, 157, 120, 170, 171, 142, 124, 1121, 106, 121, 125, 163, 107, 143, 168, 109, 148, 108, 118, 123, 1221, 169,
    149, 152, 119, 122, 162, 1231, 128, 132, 173, 172, 179, 178, 129, 133, 153, 1131, 110, 144, 159, 126, 131, 158,
    111, 113, 112, 165, 127, 145, 130, 164, 136, 140, 137, 141, 180, 181, 134, 139, 160, 161, 135, 138,
)


def wanted(step):
    if step < 1000:
        _, src, _, pieces = PLAN.msgs[step]
        if pieces is None:
            return [src]
        n = src[2] // len(pieces)
        return [(buf, row, n) for terms in pieces for buf, row in terms]
    if step < 1100:
        (i, m), (t, n) = IMG_CHUNKS[step // 10 % 10], TXT_CHUNKS[step % 10]
        return [("img", i, m), ("txt", t, n)]
    return []


def group_waits():
    group, rows = {}, []
    steps = [wanted(step) for step in ORDER]
    steps += [[(buf, row, UNIT) for _, terms in final for buf, row in terms] for final in (PLAN.final_img, PLAN.final_txt)]
    for regions in steps:
        new = []
        for buf, row, n in regions:
            for r in range(row, row + n):
                index = PLAN.origin.get((buf, r))
                if index is not None and buf not in ("iid", "tid") and index not in group and index not in new:
                    new.append(index)
        for index in new:
            group[index] = len(rows)
        if new:
            rows.append(sum(PLAN.msgs[index][2][2] for index in new))
    for index in range(len(PLAN.msgs)):
        if index not in group:
            group[index] = len(rows)
            rows.append(0)
    return group, rows


GROUP, GROUP_ROWS = group_waits()


def unit_rows(v):
    v = v.astype(F32)
    inv = lax.rsqrt(jnp.sum(v * v, axis=1, keepdims=True) + 1e-6)
    return v * inv, inv


def kernel(ie_ref, te_ref, ii_ref, ti_ref, oi_ref, ot_ref,
           ie, te, ids, img, txt, coef, gi, gt, sb, rb, iid, tid, icol, ssem, rsem, isem):
    blk, rep, sub = lax.axis_index("blk"), lax.axis_index("rep"), lax.axis_index("sub")
    where = {
        "x+": {"sub": lax.rem(sub + 1, 4)}, "x-": {"sub": lax.rem(sub + 3, 4)},
        "y+": {"blk": lax.rem(blk + 2, 8)}, "y-": {"blk": lax.rem(blk + 6, 8)},
        "z+": {"rep": lax.rem(rep + 1, 8)}, "z-": {"rep": lax.rem(rep + 7, 8)},
        "c": {"blk": blk + 1 - 2 * lax.rem(blk, 2)},
    }
    barrier = pltpu.get_barrier_semaphore()
    for way in where.values():
        pl.semaphore_signal(barrier, inc=1, device_id=way, device_id_type=MESH)
    loads = [
        pltpu.make_async_copy(src, dst, isem.at[k])
        for k, (src, dst) in enumerate(((ie_ref, ie), (te_ref, te), (ii_ref, ids.at[0]), (ti_ref, ids.at[1])))
    ]
    for load in loads:
        load.start()
    for load in loads:
        load.wait()
    img[pl.ds(img_row(0, 0), ROWS), :] = unit_rows(ie[...])[0].astype(BF16)
    txt[pl.ds(txt_row(0, 0), ROWS), :] = unit_rows(te[...])[0].astype(BF16)
    for k, ref, row in ((0, iid, iid_row(0)), (1, tid, tid_row(0, 0))):
        ref[row] = jnp.concatenate([ids[k], ids[k]], axis=1)
    pl.semaphore_wait(barrier, len(where))

    bufs = {"img": img, "txt": txt, "gi": gi, "gt": gt, "sb": sb, "rb": rb, "iid": iid, "tid": tid}

    def copy(index):
        way, src, dst, _ = PLAN.msgs[index]
        return pltpu.make_async_remote_copy(
            src_ref=bufs[src[0]].at[pl.ds(src[1], src[2])],
            dst_ref=bufs[dst[0]].at[pl.ds(dst[1], dst[2])],
            send_sem=ssem.at[("iid", "img", "sb").index(KIND[src[0]])], recv_sem=rsem.at[GROUP[index]],
            device_id=where[way], device_id_type=MESH,
        )

    here, sent = set(), []

    def need(buf, row, n):
        for r in range(row, row + n):
            name = PLAN.origin.get((buf, r))
            if name is not None and name not in here:
                g = GROUP[name]
                here.update(k for k in GROUP if GROUP[k] == g)
                if GROUP_ROWS[g]:
                    whole = rb.at[pl.ds(0, GROUP_ROWS[g])]
                    pltpu.make_async_copy(whole, whole, rsem.at[g]).wait()
                else:
                    copy(name).wait_recv()

    def total(n, terms):
        acc = None
        for buf, row in terms:
            need(buf, row, n)
            v = bufs[buf][pl.ds(row, n), :].astype(F32)
            acc = v if acc is None else acc + v
        return acc

    def send(name):
        _, src, _, pieces = PLAN.msgs[name]
        if pieces is None:
            need(*src)
        else:
            n = src[2] // len(pieces)
            for k, terms in enumerate(pieces):
                sb[pl.ds(src[1] + n * k, n), :] = total(n, terms).astype(BF16)
        copy(name).start()
        sent.append(name)

    lane = lax.broadcasted_iota(jnp.int32, (1, 128), 1)
    ready = set()

    def columns(row, n):
        for p in range(row // 128, (row + n) // 128):
            if p not in ready:
                ready.add(p)
                need("iid", 2 * p, 2)
                both_ids = jnp.where(lane < 64, iid[2 * p], iid[2 * p + 1])
                icol[pl.ds(128 * p, 128), :] = jnp.transpose(jnp.broadcast_to(both_ids, (128, 128)))

    def tile(i, m, t, n):
        need("img", i, m)
        need("txt", t, n)
        columns(i, m)
        keys = []
        for b in range(t // 64, (t + n) // 64, 2):
            r0, r1 = tid_row(*T_ORDER[b]), tid_row(*T_ORDER[b + 1])
            need("tid", r0, 1)
            need("tid", r1, 1)
            keys.append(jnp.where(lane < 64, tid[r0], tid[r1]))
        z = lax.dot_general(img[pl.ds(i, m), :], txt[pl.ds(t, n), :],
                            (((1,), (1,)), ((), ())), preferred_element_type=F32)
        sig = jax.nn.sigmoid(SCALE * z + BIAS)
        rows = icol[pl.ds(i, m), :]
        same = jnp.concatenate([(rows == k).astype(F32) for k in keys], axis=1)
        coef[pl.ds(i, m), pl.ds(t, n)] = (SCALE * (sig - same)).astype(BF16)

    def gradient(ref, row, n, part, g):
        rows = pl.ds(row, n)
        ref[rows, :] = ref[rows, :] + g if part else g

    for step in ORDER:
        if step < 1000:
            send(step)
            continue
        c, part = step // 10 % 10, step % 10
        if step < 1100:
            tile(*IMG_CHUNKS[c], *TXT_CHUNKS[part])
        elif step < 1200:
            (i, m), ks = IMG_CHUNKS[c], pl.ds(*TERMS[part])
            gradient(gi, i, m, part, jnp.dot(coef[pl.ds(i, m), ks], txt[ks, :], preferred_element_type=F32))
        else:
            (t, n), ks = TXT_CHUNKS[c], pl.ds(*TERMS[part])
            gradient(gt, t, n, part, lax.dot_general(coef[ks, pl.ds(t, n)], img[ks, :], (((0,), (0,)), ((), ())),
                                                     preferred_element_type=F32))
    for pieces, out in ((PLAN.final_img, oi_ref), (PLAN.final_txt, ot_ref)):
        for row, terms in pieces:
            out[pl.ds(row, UNIT), :] = total(UNIT, terms)
    n_msgs = len(PLAN.msgs)
    assert len(sent) == n_msgs and len(here) == n_msgs
    for kind, ref in (("iid", tid), ("img", sb), ("sb", sb)):
        n = sum(src[2] for _, src, _, _ in PLAN.msgs if KIND[src[0]] == kind)
        k = ("iid", "img", "sb").index(kind)
        pltpu.make_async_copy(ref.at[pl.ds(0, n)], ref.at[pl.ds(0, n)], ssem.at[k]).wait()


def project(ie_ref, te_ref, gi_ref, gt_ref, oi_ref, ot_ref):
    for embed, grad, out in ((ie_ref, gi_ref, oi_ref), (te_ref, gt_ref, ot_ref)):
        unit, inv = unit_rows(embed[...])
        g = grad[...]
        along = jnp.sum(unit * g, axis=1, keepdims=True)
        out[...] = (g - unit * along) * inv


def body(image_embed, text_embed, image_ids, text_ids):
    vmem, hbm = pl.BlockSpec(memory_space=pltpu.VMEM), pl.BlockSpec(memory_space=pltpu.HBM)
    out = jax.ShapeDtypeStruct((ROWS, D), F32)
    sums = pl.pallas_call(
        kernel,
        name="pairs",
        out_shape=(out, out),
        in_specs=[hbm] * 4,
        out_specs=(vmem, vmem),
        scratch_shapes=[
            pltpu.VMEM((ROWS, D), BF16),
            pltpu.VMEM((ROWS, D), BF16),
            pltpu.VMEM((2, 1, ROWS), jnp.int32),
            pltpu.VMEM((1024, D), BF16),
            pltpu.VMEM((1024, D), BF16),
            pltpu.VMEM((1024, 1024), BF16),
            pltpu.VMEM((1024, D), F32),
            pltpu.VMEM((1024, D), F32),
            pltpu.VMEM((PLAN.rows["sb"], D), BF16),
            pltpu.VMEM((PLAN.rows["rb"], D), BF16),
            pltpu.VMEM((16, 1, 128), jnp.int32),
            pltpu.VMEM((32, 1, 128), jnp.int32),
            pltpu.VMEM((1024, 128), jnp.int32),
            pltpu.SemaphoreType.DMA((3,)),
            pltpu.SemaphoreType.DMA((len(GROUP_ROWS),)),
            pltpu.SemaphoreType.DMA((4,)),
        ],
        compiler_params=pltpu.CompilerParams(
            collective_id=0, has_side_effects=True, vmem_limit_bytes=48 * 1024 * 1024
        ),
    )(*(pltpu.with_memory_space_constraint(a, pltpu.HBM)
        for a in (image_embed, text_embed, image_ids.reshape(1, ROWS), text_ids.reshape(1, ROWS))))
    return pl.pallas_call(
        project,
        name="project",
        out_shape=(out, out),
        in_specs=[vmem] * 4,
        out_specs=(vmem, vmem),
        compiler_params=pltpu.CompilerParams(vmem_limit_bytes=4 * 1024 * 1024),
    )(image_embed, text_embed, *sums)


def solution(mesh):
    rows = P(("blk", "rep", "sub"), None)
    flat = P(("blk", "rep", "sub"))
    return jax.shard_map(
        body, mesh=mesh, in_specs=(rows, rows, flat, flat), out_specs=(rows, rows), check_vma=False
    )
```

```python
import jax
import jax.numpy as jnp
from jax import lax
from jax.experimental import pallas as pl
from jax.experimental.pallas import tpu as pltpu
from jax.sharding import PartitionSpec as P

SCALE = 30.0
BIAS = -3.0
ROWS = 64
D = 1152
UNIT = 16
GATHER_XY, REDUCE_XY = 32, 32
PARTS_Z = {1: ((0, 16), (16, 16), (32, 16), (48, 16)), -1: ((48, 16), (32, 16), (16, 16), (0, 16))}
IMG_CHUNKS = ((0, 256), (256, 256), (512, 256), (768, 256))
TXT_CHUNKS = ((0, 256), (256, 256), (512, 256), (768, 256))
TERMS = ((512, 512), (0, 512))
MESH = pl.DeviceIdType.MESH
F32 = jnp.float32
BF16 = jnp.bfloat16

Z_ORDER = (4, 3, -3, 2, -2, 1, -1, 0)
T_ORDER = (
    (2, 2), (1, 2), (2, 1), (-1, 2), (2, -1), (0, 2), (2, 0), (1, 1),
    (-1, 1), (1, -1), (-1, -1), (0, 1), (1, 0), (0, -1), (-1, 0), (0, 0),
)
RING4 = (0, 1, -1, 2)


def near4(d):
    return (d + 1) % 4 - 1


def near8(d):
    return (d + 3) % 8 - 3


def img_row(lane, dz):
    return Z_ORDER.index(near8(dz)) * 128 + lane * 64


def txt_row(dx, dy):
    return T_ORDER.index((near4(dx), near4(dy))) * 64


def tid_row(dx, dy):
    return RING4.index(near4(dy)) * 4 + RING4.index(near4(dx))


def iid_row(dz):
    return Z_ORDER.index(near8(dz)) * 2


class Plan:
    def __init__(self):
        self.msgs = []
        self.origin = {}
        self.rows = {"sb": 0, "rb": 0}

    def add(self, way, src, dst, pieces=None):
        buf, row, n = dst
        for r in range(row, row + n):
            assert (buf, r) not in self.origin
            self.origin[buf, r] = len(self.msgs)
        self.msgs.append((way, src, dst, pieces))

    def room(self, buf, n):
        row = self.rows[buf]
        self.rows[buf] += n
        return row

    def reduce(self, way, n, *pieces):
        src, dst = self.room("sb", n), self.room("rb", n)
        self.add(way, ("sb", src, n), ("rb", dst, n), pieces)
        return dst


SIDES = ((1, "+"), (-1, "-"))
HALVES = ((0, "x", "y", lambda u, v: txt_row(u, v)), (32, "y", "x", lambda u, v: txt_row(v, u)))


def make_plan():
    p = Plan()
    p.add("c", ("iid", iid_row(0), 1), ("iid", iid_row(0) + 1, 1))
    for k in range(4):
        p.add("z+", ("iid", iid_row(-k), 2), ("iid", iid_row(-k - 1), 2))
        if k < 3:
            p.add("z-", ("iid", iid_row(k), 2), ("iid", iid_row(k + 1), 2))
    p.add("x+", ("tid", tid_row(0, 0), 1), ("tid", tid_row(-1, 0), 1))
    p.add("x-", ("tid", tid_row(0, 0), 1), ("tid", tid_row(1, 0), 1))
    p.add("x+", ("tid", tid_row(-1, 0), 1), ("tid", tid_row(2, 0), 1))
    p.add("y+", ("tid", tid_row(0, 0), 4), ("tid", tid_row(0, -1), 4))
    p.add("y-", ("tid", tid_row(0, 0), 4), ("tid", tid_row(0, 1), 4))
    p.add("y+", ("tid", tid_row(0, -1), 4), ("tid", tid_row(0, 2), 4))
    for k in range(4):
        for s, w in SIDES:
            for q, n in PARTS_Z[s]:
                if k < 3 or (q < 32) == (s == 1):
                    p.add("z" + w, ("img", img_row(0, -s * k) + q, n), ("img", img_row(0, -s * (k + 1)) + q, n))
    for dz in Z_ORDER:
        for h in (0, 1):
            p.add("c", ("img", img_row(0, dz) + 32 * h, 32), ("img", img_row(1, dz) + 32 * h, 32))
    for o, one, two, at in HALVES:
        n = GATHER_XY
        for s, w in SIDES:
            for q in range(0, 32, n):
                p.add(one + w, ("txt", at(0, 0) + o + q, n), ("txt", at(-s, 0) + o + q, n))
                for u in RING4:
                    p.add(two + w, ("txt", at(u, 0) + o + q, n), ("txt", at(u, -s) + o + q, n))
            e = o if s == 1 else o + UNIT
            p.add(one + w, ("txt", at(-s, 0) + e, UNIT), ("txt", at(2, 0) + e, UNIT))
            for u in RING4:
                p.add(two + w, ("txt", at(u, -s) + e, UNIT), ("txt", at(u, 2) + e, UNIT))
    part = {}
    for dz in Z_ORDER:
        for h in (0, 1):
            row = p.reduce("c", 32, [("gi", img_row(1, dz) + 32 * h)])
            part[dz, 2 * h], part[dz, 2 * h + 1] = row, row + UNIT
    got = {}
    for j in (4, 3, 2, 1):
        for s, w in SIDES:
            for q, n in PARTS_Z[s]:
                if j == 4 and (q < 32) != (s == 1):
                    continue
                dz, pieces = near8(s * j), []
                for e in range(q // UNIT, (q + n) // UNIT):
                    terms = [("gi", img_row(0, dz) + UNIT * e), ("rb", part[dz, e])]
                    if (s, j, e) in got:
                        terms.append(("rb", got[s, j, e]))
                    pieces.append(terms)
                row = p.reduce("z" + w, n, *pieces)
                for k in range(n // UNIT):
                    got[s, j - 1, q // UNIT + k] = row + UNIT * k
    p.final_img = [
        (UNIT * q, [("gi", img_row(0, 0) + UNIT * q), ("rb", part[0, q]), ("rb", got[1, 0, q]), ("rb", got[-1, 0, q])])
        for q in range(4)
    ]
    p.final_txt = []
    for o, one, two, at in HALVES:
        n = REDUCE_XY
        base = {}
        for u in RING4:
            far, last = {}, {}
            for s, w in SIDES:
                q = 0 if s == 1 else 1
                far[s, q] = p.reduce(two + w, UNIT, [("gt", at(u, 2) + o + UNIT * q)])
            for s, w in SIDES:
                for q in range(0, 2, n // UNIT):
                    pieces = [[("gt", at(u, s) + o + UNIT * e)] + ([("rb", far[s, e])] if (s, e) in far else [])
                              for e in range(q, q + n // UNIT)]
                    row = p.reduce(two + w, n, *pieces)
                    for k in range(n // UNIT):
                        last[s, q + k] = row + UNIT * k
            for q in (0, 1):
                base[u, q] = [("gt", at(u, 0) + o + UNIT * q), ("rb", last[1, q]), ("rb", last[-1, q])]
        far, last = {}, {}
        for s, w in SIDES:
            q = 0 if s == 1 else 1
            far[s, q] = p.reduce(one + w, UNIT, base[2, q])
        for s, w in SIDES:
            for q in range(0, 2, n // UNIT):
                pieces = [base[s, e] + ([("rb", far[s, e])] if (s, e) in far else []) for e in range(q, q + n // UNIT)]
                row = p.reduce(one + w, n, *pieces)
                for k in range(n // UNIT):
                    last[s, q + k] = row + UNIT * k
        for q in (0, 1):
            p.final_txt.append((o + UNIT * q, base[0, q] + [("rb", last[1, q]), ("rb", last[-1, q])]))
    return p


PLAN = make_plan()
KIND = {"iid": "iid", "tid": "iid", "img": "img", "txt": "img", "sb": "sb"}

ORDER = (
    78, 58, 88, 68, 15, 18, 0, 57, 56, 16, 19, 59, 8, 69, 9, 79, 89, 14, 20, 1, 21, 17, 2, 23, 26, 83, 63, 93, 73,
    24, 27, 53, 60, 10, 70, 90, 80, 22, 28, 54, 3, 29, 52, 25, 61, 55, 71, 91, 81, 4, 31, 34, 11, 72, 92, 32, 35,
    82, 62, 49, 30, 36, 50, 5, 12, 95, 85, 65, 75, 37, 48, 51, 33, 6, 94, 84, 64, 74, 39, 40, 1023, 41, 13, 66, 45,
    76, 86, 96, 1033, 1230, 38, 46, 77, 97, 87, 67, 1032, 7, 1022, 44, 47, 1120, 1220, 1130, 1012, 1013, 43, 1110,
    1011, 42, 1021, 1031, 1020, 1030, 1200, 1000, 1010, 1201, 175, 174, 154, 155, 1003, 167, 166, 146, 147, 1001,
    1002, 1100, 150, 151, 1101, 98, 99, 100, 101, 1111, 105, 104, 102, 103, 114, 117, 177, 176, 156, 115, 116, 1210,
    1211, 157, 120, 170, 171, 142, 124, 1121, 106, 121, 125, 163, 107, 143, 168, 109, 148, 108, 118, 123, 1221, 169,
    149, 152, 119, 122, 162, 1231, 128, 132, 173, 172, 179, 178, 129, 133, 153, 1131, 110, 144, 159, 126, 131, 158,
    111, 113, 112, 165, 127, 145, 130, 164, 136, 140, 137, 141, 180, 181, 134, 139, 160, 161, 135, 138,
)


def wanted(step):
    if step < 1000:
        _, src, _, pieces = PLAN.msgs[step]
        if pieces is None:
            return [src]
        n = src[2] // len(pieces)
        return [(buf, row, n) for terms in pieces for buf, row in terms]
    if step < 1100:
        (i, m), (t, n) = IMG_CHUNKS[step // 10 % 10], TXT_CHUNKS[step % 10]
        return [("img", i, m), ("txt", t, n)]
    return []


def group_waits():
    group, rows = {}, []
    steps = [wanted(step) for step in ORDER]
    steps += [[(buf, row, UNIT) for _, terms in final for buf, row in terms] for final in (PLAN.final_img, PLAN.final_txt)]
    for regions in steps:
        new = []
        for buf, row, n in regions:
            for r in range(row, row + n):
                index = PLAN.origin.get((buf, r))
                if index is not None and buf not in ("iid", "tid") and index not in group and index not in new:
                    new.append(index)
        for index in new:
            group[index] = len(rows)
        if new:
            rows.append(sum(PLAN.msgs[index][2][2] for index in new))
    for index in range(len(PLAN.msgs)):
        if index not in group:
            group[index] = len(rows)
            rows.append(0)
    return group, rows


GROUP, GROUP_ROWS = group_waits()


def unit_rows(v):
    v = v.astype(F32)
    inv = lax.rsqrt(jnp.sum(v * v, axis=1, keepdims=True) + 1e-6)
    return v * inv, inv


def kernel(ie_ref, te_ref, ii_ref, ti_ref, oi_ref, ot_ref,
           ie, te, ids, img, txt, coef, gi, gt, sb, rb, iid, tid, icol, ssem, rsem, isem):
    blk, rep, sub = lax.axis_index("blk"), lax.axis_index("rep"), lax.axis_index("sub")
    where = {
        "x+": {"sub": lax.rem(sub + 1, 4)}, "x-": {"sub": lax.rem(sub + 3, 4)},
        "y+": {"blk": lax.rem(blk + 2, 8)}, "y-": {"blk": lax.rem(blk + 6, 8)},
        "z+": {"rep": lax.rem(rep + 1, 8)}, "z-": {"rep": lax.rem(rep + 7, 8)},
        "c": {"blk": blk + 1 - 2 * lax.rem(blk, 2)},
    }
    barrier = pltpu.get_barrier_semaphore()
    for way in where.values():
        pl.semaphore_signal(barrier, inc=1, device_id=way, device_id_type=MESH)
    loads = [
        pltpu.make_async_copy(src, dst, isem.at[k])
        for k, (src, dst) in enumerate(((ie_ref, ie), (te_ref, te), (ii_ref, ids.at[0]), (ti_ref, ids.at[1])))
    ]
    for load in loads:
        load.start()
    for load in loads:
        load.wait()
    img[pl.ds(img_row(0, 0), ROWS), :] = unit_rows(ie[...])[0].astype(BF16)
    txt[pl.ds(txt_row(0, 0), ROWS), :] = unit_rows(te[...])[0].astype(BF16)
    for k, ref, row in ((0, iid, iid_row(0)), (1, tid, tid_row(0, 0))):
        ref[row] = jnp.concatenate([ids[k], ids[k]], axis=1)
    pl.semaphore_wait(barrier, len(where))

    bufs = {"img": img, "txt": txt, "gi": gi, "gt": gt, "sb": sb, "rb": rb, "iid": iid, "tid": tid}

    def copy(index):
        way, src, dst, _ = PLAN.msgs[index]
        return pltpu.make_async_remote_copy(
            src_ref=bufs[src[0]].at[pl.ds(src[1], src[2])],
            dst_ref=bufs[dst[0]].at[pl.ds(dst[1], dst[2])],
            send_sem=ssem.at[("iid", "img", "sb").index(KIND[src[0]])], recv_sem=rsem.at[GROUP[index]],
            device_id=where[way], device_id_type=MESH,
        )

    here, sent = set(), []

    def need(buf, row, n):
        for r in range(row, row + n):
            name = PLAN.origin.get((buf, r))
            if name is not None and name not in here:
                g = GROUP[name]
                here.update(k for k in GROUP if GROUP[k] == g)
                if GROUP_ROWS[g]:
                    whole = rb.at[pl.ds(0, GROUP_ROWS[g])]
                    pltpu.make_async_copy(whole, whole, rsem.at[g]).wait()
                else:
                    copy(name).wait_recv()

    def total(n, terms):
        acc = None
        for buf, row in terms:
            need(buf, row, n)
            v = bufs[buf][pl.ds(row, n), :].astype(F32)
            acc = v if acc is None else acc + v
        return acc

    def send(name):
        _, src, _, pieces = PLAN.msgs[name]
        if pieces is None:
            need(*src)
        else:
            n = src[2] // len(pieces)
            for k, terms in enumerate(pieces):
                sb[pl.ds(src[1] + n * k, n), :] = total(n, terms).astype(BF16)
        copy(name).start()
        sent.append(name)

    lane = lax.broadcasted_iota(jnp.int32, (1, 128), 1)
    ready = set()

    def columns(row, n):
        for p in range(row // 128, (row + n) // 128):
            if p not in ready:
                ready.add(p)
                need("iid", 2 * p, 2)
                both_ids = jnp.where(lane < 64, iid[2 * p], iid[2 * p + 1])
                icol[pl.ds(128 * p, 128), :] = jnp.transpose(jnp.broadcast_to(both_ids, (128, 128)))

    def tile(i, m, t, n):
        need("img", i, m)
        need("txt", t, n)
        columns(i, m)
        keys = []
        for b in range(t // 64, (t + n) // 64, 2):
            r0, r1 = tid_row(*T_ORDER[b]), tid_row(*T_ORDER[b + 1])
            need("tid", r0, 1)
            need("tid", r1, 1)
            keys.append(jnp.where(lane < 64, tid[r0], tid[r1]))
        z = lax.dot_general(img[pl.ds(i, m), :], txt[pl.ds(t, n), :],
                            (((1,), (1,)), ((), ())), preferred_element_type=F32)
        sig = jax.nn.sigmoid(SCALE * z + BIAS)
        rows = icol[pl.ds(i, m), :]
        same = jnp.concatenate([(rows == k).astype(F32) for k in keys], axis=1)
        coef[pl.ds(i, m), pl.ds(t, n)] = (SCALE * (sig - same)).astype(BF16)

    def gradient(ref, row, n, part, g):
        rows = pl.ds(row, n)
        ref[rows, :] = ref[rows, :] + g if part else g

    for step in ORDER:
        if step < 1000:
            send(step)
            continue
        c, part = step // 10 % 10, step % 10
        if step < 1100:
            tile(*IMG_CHUNKS[c], *TXT_CHUNKS[part])
        elif step < 1200:
            (i, m), ks = IMG_CHUNKS[c], pl.ds(*TERMS[part])
            gradient(gi, i, m, part, jnp.dot(coef[pl.ds(i, m), ks], txt[ks, :], preferred_element_type=F32))
        else:
            (t, n), ks = TXT_CHUNKS[c], pl.ds(*TERMS[part])
            gradient(gt, t, n, part, lax.dot_general(coef[ks, pl.ds(t, n)], img[ks, :], (((0,), (0,)), ((), ())),
                                                     preferred_element_type=F32))
    for pieces, out in ((PLAN.final_img, oi_ref), (PLAN.final_txt, ot_ref)):
        for row, terms in pieces:
            out[pl.ds(row, UNIT), :] = total(UNIT, terms)
    n_msgs = len(PLAN.msgs)
    assert len(sent) == n_msgs and len(here) == n_msgs
    for kind, ref in (("iid", tid), ("img", sb), ("sb", sb)):
        n = sum(src[2] for _, src, _, _ in PLAN.msgs if KIND[src[0]] == kind)
        k = ("iid", "img", "sb").index(kind)
        pltpu.make_async_copy(ref.at[pl.ds(0, n)], ref.at[pl.ds(0, n)], ssem.at[k]).wait()


def project(ie_ref, te_ref, gi_ref, gt_ref, oi_ref, ot_ref, made, sem):
    writes = []
    for k, (embed, grad, out) in enumerate(((ie_ref, gi_ref, oi_ref), (te_ref, gt_ref, ot_ref))):
        unit, inv = unit_rows(embed[...])
        g = grad[...]
        along = jnp.sum(unit * g, axis=1, keepdims=True)
        made[k] = (g - unit * along) * inv
        writes.append(pltpu.make_async_copy(made.at[k], out, sem.at[k]))
        writes[k].start()
    for write in writes:
        write.wait()


def body(image_embed, text_embed, image_ids, text_ids):
    vmem, hbm = pl.BlockSpec(memory_space=pltpu.VMEM), pl.BlockSpec(memory_space=pltpu.HBM)
    out = jax.ShapeDtypeStruct((ROWS, D), F32)
    sums = pl.pallas_call(
        kernel,
        name="pairs",
        out_shape=(out, out),
        in_specs=[hbm] * 4,
        out_specs=(vmem, vmem),
        scratch_shapes=[
            pltpu.VMEM((ROWS, D), BF16),
            pltpu.VMEM((ROWS, D), BF16),
            pltpu.VMEM((2, 1, ROWS), jnp.int32),
            pltpu.VMEM((1024, D), BF16),
            pltpu.VMEM((1024, D), BF16),
            pltpu.VMEM((1024, 1024), BF16),
            pltpu.VMEM((1024, D), F32),
            pltpu.VMEM((1024, D), F32),
            pltpu.VMEM((PLAN.rows["sb"], D), BF16),
            pltpu.VMEM((PLAN.rows["rb"], D), BF16),
            pltpu.VMEM((16, 1, 128), jnp.int32),
            pltpu.VMEM((32, 1, 128), jnp.int32),
            pltpu.VMEM((1024, 128), jnp.int32),
            pltpu.SemaphoreType.DMA((3,)),
            pltpu.SemaphoreType.DMA((len(GROUP_ROWS),)),
            pltpu.SemaphoreType.DMA((4,)),
        ],
        compiler_params=pltpu.CompilerParams(
            collective_id=0, has_side_effects=True, vmem_limit_bytes=48 * 1024 * 1024
        ),
    )(*(pltpu.with_memory_space_constraint(a, pltpu.HBM)
        for a in (image_embed, text_embed, image_ids.reshape(1, ROWS), text_ids.reshape(1, ROWS))))
    return pl.pallas_call(
        project,
        name="project",
        out_shape=(out, out),
        in_specs=[vmem] * 4,
        out_specs=(hbm, hbm),
        scratch_shapes=[pltpu.VMEM((2, ROWS, D), F32), pltpu.SemaphoreType.DMA((2,))],
        compiler_params=pltpu.CompilerParams(vmem_limit_bytes=4 * 1024 * 1024),
    )(image_embed, text_embed, *sums)


def solution(mesh):
    rows = P(("blk", "rep", "sub"), None)
    flat = P(("blk", "rep", "sub"))
    return jax.shard_map(
        body, mesh=mesh, in_specs=(rows, rows, flat, flat), out_specs=(rows, rows), check_vma=False
    )
```
